32 devices in a mesh: fields: 2 (over x), rows: 16 (over z, y, core).
Axes of the slice: x: 2, y: 2, z: 4, core: 2. Of those that a mesh axis runs over, the one named last changes fastest.
Arguments:
- members: bfloat16 [512, 131072], P('rows', 'fields'), parts along dimension 1, may hold values from -6 to 6
- predicted: bfloat16 [512, 32768], P('rows', 'fields'), parts along dimension 1, may hold values from -6 to 6
- noise: bfloat16 [512, 32768], P('rows', 'fields'), parts along dimension 1, may hold values from -6 to 6
- observed: float32 [32768], P(('fields', 'rows')), parts along dimension 0, may hold values from -12 to 12
- observation_spread: float32 [32768], P(('fields', 'rows')), parts along dimension 0, may hold values from 1 to 16
Outputs:
- updated: bfloat16 [512, 131072], P('rows', 'fields'), parts along dimension 1
The draws below stay inside these ranges and needn't reach their ends.
There are 2 independent parts, one for each index of `fields`. The reference program is written for one: setup_inputs(seed, part) draws one part's arguments, and reference() takes and returns one part's arrays. A program takes and returns all parts, laid end to end along the dimension named above; each array names one. Nothing has to cross between parts.
All inputs are finite; a program needn't handle non-finite values.
Results may differ from the reference program's by a relative error of at most 0.005.
Values may be sent and summed in bfloat16 or wider, within the bound.
A program may use at most 64 MiB of HBM per device.

```python
import math
import jax
import jax.numpy as jnp
from jax import lax

NE = 512
NC = 65536
ND = 16384


def with_spikes(values, key, source, target, blocks, factor):
    def block_of(position):
        return (jnp.arange(values.shape[position]) // (values.shape[position] // blocks)).reshape((-1,) + (1,) * (values.ndim - 1 - position))

    near = jax.random.permutation(key, blocks)[block_of(target)]
    far = (block_of(target) + blocks // 2) % blocks
    return jnp.where((block_of(source) == near) | (block_of(source) == far), factor * values, values)


def shard_levels(own_key, shape, split, least, largest):
    def one(dim, blocks):
        steps = jax.random.uniform(jax.random.fold_in(jax.random.fold_in(own_key, 6), dim), (blocks,), jnp.float32, least / len(split), largest / len(split))
        return jnp.repeat(jnp.exp(steps), shape[dim] // blocks).reshape((-1,) + (1,) * (len(shape) - dim - 1))

    level = one(*split[0])
    for cut in split[1:]:
        level = level * one(*cut)
    return level


def bell_draw(key, shape, deviation, limit, split=(), held_as=jnp.bfloat16):
    array = deviation * jax.random.normal(key, shape, jnp.float32)
    if split:
        array = array * shard_levels(key, shape, split, -0.22, 0.18)
    return jnp.clip(array, -limit, limit).astype(held_as)


def gaussian_with(stream_key, shape, deviation, limit, shards, heavy, kind=jnp.bfloat16):
    result = deviation * jax.random.normal(stream_key, shape, jnp.float32)
    if shards:
        result = result * shard_levels(stream_key, shape, shards, -0.22, 0.18)
    return jnp.clip(with_spikes(result, jax.random.fold_in(stream_key, 3), *heavy), -limit, limit).astype(kind)


def setup_inputs(seed: int = 0, part: int = 0) -> dict:
    seeds = jax.random.split(jax.random.key(seed), 6)
    own_keys = jax.random.split(jax.random.fold_in(seeds[5], part), 6)
    return {
        "members": bell_draw(own_keys[0], (NE, NC), 1.0, 6.0, ((0, 16),)),
        "predicted": gaussian_with(own_keys[1], (NE, ND), 1.0, 6.0, ((0, 16),), (1, 0, 16, 2.0)),
        "noise": bell_draw(own_keys[2], (NE, ND), 1.0, 6.0, ((0, 16),)),
        "observed": bell_draw(own_keys[3], (ND,), 2.0, 12.0, ((0, 16),), jnp.float32),
        "observation_spread": jnp.clip(jnp.exp(math.log(16.0) - 2.7725887 * jax.random.uniform(own_keys[4], (ND,), jnp.float32) ** shard_levels(own_keys[4], (ND,), ((0, 16),), -0.2, 0.2)), 1.0, 16.0),
    }


damping = 21.0

def reference(members, predicted, noise, observed, observation_spread):
    inverse_square_root = 1.0 / math.sqrt(NE - 1)
    predicted_response = predicted.astype(jnp.float32)
    ensemble_data_average = lax.optimization_barrier(jnp.mean(predicted_response, axis=0))
    standardized_anomalies = ((predicted_response - ensemble_data_average) * (inverse_square_root / observation_spread)).astype(jnp.bfloat16)
    measurement_residual = ((observed - predicted_response) / observation_spread + noise.astype(jnp.float32)).astype(jnp.bfloat16)
    gram_matrix = lax.dot_general(standardized_anomalies.astype(jnp.float32), standardized_anomalies.astype(jnp.float32), (((1,), (1,)), ((), ())), preferred_element_type=jnp.float32)
    cross_terms = lax.dot_general(standardized_anomalies.astype(jnp.float32), measurement_residual.astype(jnp.float32), (((1,), (1,)), ((), ())), preferred_element_type=jnp.float32)
    system = gram_matrix + damping * jnp.eye(NE, dtype=jnp.float32)
    factor = jnp.linalg.cholesky(system)
    weights = jax.scipy.linalg.cho_solve((factor, True), cross_terms).astype(jnp.bfloat16)
    params = members.astype(jnp.float32)
    cell_mean = lax.optimization_barrier(jnp.mean(params, axis=0))
    anomaly = ((params - cell_mean) * inverse_square_root).astype(jnp.bfloat16)
    update = lax.dot_general(weights.astype(jnp.float32), anomaly.astype(jnp.float32), (((0,), (0,)), ((), ())), preferred_element_type=jnp.float32)
    return (params + update).astype(jnp.bfloat16)
```

```python
import functools
import math

import jax
import jax.numpy as jnp
from jax import lax
from jax.experimental import pallas as pl
from jax.experimental.pallas import tpu as pltpu
from jax.sharding import PartitionSpec as P

damping = 21.0
BLOCK = 128
HIGHEST = lax.Precision.HIGHEST


def sweep_block(m):
    size = m.shape[0]
    rows = lax.broadcasted_iota(jnp.int32, m.shape, 0)
    columns = lax.broadcasted_iota(jnp.int32, m.shape, 1)
    for k in range(size):
        row = m[k : k + 1, :]
        column = m[:, k : k + 1]
        inverse = 1.0 / m[k : k + 1, k : k + 1]
        scaled = row * inverse
        swept = m - column * scaled
        swept = jnp.where(columns == k, column * inverse, swept)
        edge = jnp.where(columns[k : k + 1] == k, -inverse, scaled)
        m = jnp.where(rows == k, edge, swept)
    return m


def solve_kernel(gram_ref, cross_t_ref, weights_t_ref, a_ref):
    ne = gram_ref.shape[0]
    eye = lax.broadcasted_iota(jnp.int32, (ne, ne), 0) == lax.broadcasted_iota(
        jnp.int32, (ne, ne), 1
    )
    a_ref[...] = gram_ref[...] + jnp.where(eye, damping, 0.0)

    def step(block, carry):
        here = pl.ds(pl.multiple_of(block * BLOCK, BLOCK), BLOCK)
        negative = sweep_block(a_ref[here, here])
        panel = a_ref[here, :]
        column = a_ref[:, here]
        scaled = -jnp.dot(negative, panel, precision=HIGHEST, preferred_element_type=jnp.float32)
        scaled_column = -jnp.dot(
            column, negative, precision=HIGHEST, preferred_element_type=jnp.float32
        )
        a_ref[...] = a_ref[...] - jnp.dot(
            column, scaled, precision=HIGHEST, preferred_element_type=jnp.float32
        )
        a_ref[here, :] = scaled
        a_ref[:, here] = scaled_column
        a_ref[here, here] = negative
        return carry

    lax.fori_loop(0, ne // BLOCK, step, 0)
    weights_t_ref[...] = (
        -jnp.dot(cross_t_ref[...], a_ref[...], precision=HIGHEST, preferred_element_type=jnp.float32)
    ).astype(jnp.bfloat16)


def solve(gram, cross_t):
    ne = gram.shape[0]
    return pl.pallas_call(
        solve_kernel,
        out_shape=jax.ShapeDtypeStruct((ne, ne), jnp.bfloat16),
        in_specs=[pl.BlockSpec(memory_space=pltpu.VMEM)] * 2,
        out_specs=pl.BlockSpec(memory_space=pltpu.VMEM),
        scratch_shapes=[pltpu.VMEM((ne, ne), jnp.float32)],
        compiler_params=pltpu.CompilerParams(vmem_limit_bytes=24 * 2**20),
        cost_estimate=pl.CostEstimate(
            flops=40 * ne**3, bytes_accessed=200 * 2**20, transcendentals=0
        ),
        name="solve",
    )(gram, cross_t)


def update_kernel(n, chunk, weights_t_ref, params_ref, out_ref, held, send_sem, recv_sem, own_sem):
    me = lax.axis_index("rows")
    ne, cells = params_ref.shape
    local = ne // n
    scale = 1.0 / math.sqrt(ne - 1)

    barrier = pltpu.get_barrier_semaphore()

    def greet(s, carry):
        pl.semaphore_signal(
            barrier,
            inc=1,
            device_id={"rows": lax.rem(me + s, n)},
            device_id_type=pl.DeviceIdType.MESH,
        )
        return carry

    lax.fori_loop(1, n, greet, 0)
    pl.semaphore_wait(barrier, n - 1)

    def outgoing(c, s):
        peer = lax.rem(me + s, n)
        return pltpu.make_async_remote_copy(
            src_ref=held.at[peer, :, pl.ds(pl.multiple_of(c * chunk, chunk), chunk)],
            dst_ref=out_ref.at[:, pl.ds(pl.multiple_of(me * cells + c * chunk, chunk), chunk)],
            send_sem=send_sem.at[c, s],
            recv_sem=recv_sem.at[c, s],
            device_id={"rows": peer},
            device_id_type=pl.DeviceIdType.MESH,
        )

    def own(c):
        return pltpu.make_async_copy(
            held.at[me, :, pl.ds(pl.multiple_of(c * chunk, chunk), chunk)],
            out_ref.at[:, pl.ds(pl.multiple_of(me * cells + c * chunk, chunk), chunk)],
            own_sem.at[c],
        )

    def compute(c, carry):
        here = pl.ds(pl.multiple_of(c * chunk, chunk), chunk)
        params = params_ref[:, here].astype(jnp.float32)
        mean = jnp.sum(params, axis=0, keepdims=True) * (1.0 / ne)
        anomaly = ((params - mean) * scale).astype(jnp.bfloat16)
        update = jnp.dot(weights_t_ref[...], anomaly, preferred_element_type=jnp.float32)
        held[:, :, here] = (params + update).reshape(n, local, chunk).astype(jnp.bfloat16)

        def send(s, carry):
            outgoing(c, s).start()
            return carry

        lax.fori_loop(1, n, send, 0)
        own(c).start()
        return carry

    count = cells // chunk
    lax.fori_loop(0, count, compute, 0)

    def finish(c, carry):
        def one(s, carry):
            outgoing(c, s).wait()
            return carry

        lax.fori_loop(1, n, one, 0)
        own(c).wait()
        return carry

    lax.fori_loop(0, count, finish, 0)


def update_and_send(weights_t, params, n):
    ne, cells = params.shape
    local = ne // n
    chunk = cells
    while chunk % 2 == 0 and chunk > 512:
        chunk //= 2
    count = cells // chunk
    return pl.pallas_call(
        functools.partial(update_kernel, n, chunk),
        out_shape=jax.ShapeDtypeStruct((local, n * cells), jnp.bfloat16),
        in_specs=[pl.BlockSpec(memory_space=pltpu.VMEM)] * 2,
        out_specs=pl.BlockSpec(memory_space=pl.ANY),
        scratch_shapes=[
            pltpu.VMEM((n, local, cells), jnp.bfloat16),
            pltpu.SemaphoreType.DMA((count, n)),
            pltpu.SemaphoreType.DMA((count, n)),
            pltpu.SemaphoreType.DMA((count,)),
        ],
        compiler_params=pltpu.CompilerParams(
            collective_id=0, has_side_effects=True, vmem_limit_bytes=40 * 2**20
        ),
        name="update",
    )(weights_t, params)


def on_device(members, predicted, noise, observed, observation_spread):
    n = lax.axis_size("rows")
    local = members.shape[0]
    ne = local * n
    cells = members.shape[1] // n
    scale = 1.0 / math.sqrt(ne - 1)
    predicted, noise = (
        lax.all_to_all(predicted, "rows", split_axis=1, concat_axis=0, tiled=True),
        lax.all_to_all(noise, "rows", split_axis=1, concat_axis=0, tiled=True),
    )
    params = lax.all_to_all(members, "rows", split_axis=1, concat_axis=0, tiled=True)
    predicted = predicted.astype(jnp.float32)
    mean = jnp.mean(predicted, axis=0)
    whitened = ((predicted - mean) * (scale / observation_spread)).astype(jnp.bfloat16)
    innovation = (
        (observed - predicted) / observation_spread + noise.astype(jnp.float32)
    ).astype(jnp.bfloat16)
    both = jnp.concatenate([whitened, innovation], axis=0)
    sums = lax.dot_general(
        both, whitened, (((1,), (1,)), ((), ())), preferred_element_type=jnp.float32
    )
    sums = lax.psum(sums, "rows")
    weights_t = solve(sums[:ne], sums[ne:])
    return update_and_send(weights_t, params, n)


def solution(mesh):
    in_specs = (
        P("rows", "fields"),
        P("rows", "fields"),
        P("rows", "fields"),
        P(("fields", "rows")),
        P(("fields", "rows")),
    )
    return jax.shard_map(
        on_device, mesh=mesh, in_specs=in_specs, out_specs=P("rows", "fields"), check_vma=False
    )
```

```python
import functools
import math

import jax
import jax.numpy as jnp
from jax import lax
from jax.experimental import pallas as pl
from jax.experimental.pallas import tpu as pltpu
from jax.sharding import PartitionSpec as P

damping = 21.0
BLOCK = 128
HIGHEST = lax.Precision.HIGHEST


def sweep_block(m):
    size = m.shape[0]
    rows = lax.broadcasted_iota(jnp.int32, m.shape, 0)
    columns = lax.broadcasted_iota(jnp.int32, m.shape, 1)
    for k in range(size):
        row = m[k : k + 1, :]
        column = m[:, k : k + 1]
        inverse = 1.0 / m[k : k + 1, k : k + 1]
        scaled = row * inverse
        swept = m - column * scaled
        swept = jnp.where(columns == k, column * inverse, swept)
        edge = jnp.where(columns[k : k + 1] == k, -inverse, scaled)
        m = jnp.where(rows == k, edge, swept)
    return m


MESH = pl.DeviceIdType.MESH


def smoother_kernel(
    n,
    chunk,
    early,
    members_ref,
    predicted_ref,
    noise_ref,
    observed_ref,
    spread_ref,
    out_ref,
    response,
    jitter,
    both,
    sums,
    arrived,
    full,
    inverse,
    params_ref,
    held,
    data_send,
    data_recv,
    own_data,
    tree_send,
    tree_recv,
    member_send,
    member_recv,
    own_member,
    out_send,
    out_recv,
    own_out,
):
    me = lax.axis_index("rows")
    local = members_ref.shape[0]
    ne = n * local
    cells = members_ref.shape[1] // n
    data = predicted_ref.shape[1] // n
    count = cells // chunk
    levels = n.bit_length() - 1
    scale = 1.0 / math.sqrt(ne - 1)
    barrier = pltpu.get_barrier_semaphore()

    def each_peer(do):
        def one(s, carry):
            do(s, lax.rem(me + s, n))
            return carry

        lax.fori_loop(1, n, one, 0)

    def span(start, size):
        return pl.ds(pl.multiple_of(start, size), size)

    each_peer(
        lambda s, peer: pl.semaphore_signal(
            barrier, inc=1, device_id={"rows": peer}, device_id_type=MESH
        )
    )
    pl.semaphore_wait(barrier, n - 1)

    def remote(source, target, send, recv, peer):
        return pltpu.make_async_remote_copy(
            src_ref=source,
            dst_ref=target,
            send_sem=send,
            recv_sem=recv,
            device_id={"rows": peer},
            device_id_type=MESH,
        )

    fields = ((predicted_ref, response), (noise_ref, jitter))

    def data_copy(which, s, peer):
        source, target = fields[which]
        return remote(
            source.at[:, span(peer * data, data)],
            target.at[me],
            data_send.at[which, s],
            data_recv.at[which, s],
            peer,
        )

    def own_data_copy(which):
        source, target = fields[which]
        return pltpu.make_async_copy(
            source.at[:, span(me * data, data)], target.at[me], own_data.at[which]
        )

    def member_copy(c, s, peer):
        return remote(
            members_ref.at[:, span(peer * cells + c * chunk, chunk)],
            params_ref.at[me, :, span(c * chunk, chunk)],
            member_send.at[c, s],
            member_recv.at[c, s],
            peer,
        )

    def own_member_copy(c):
        return pltpu.make_async_copy(
            members_ref.at[:, span(me * cells + c * chunk, chunk)],
            params_ref.at[me, :, span(c * chunk, chunk)],
            own_member.at[c],
        )

    def out_copy(c, s, peer):
        return remote(
            held.at[peer, :, span(c * chunk, chunk)],
            out_ref.at[:, span(me * cells + c * chunk, chunk)],
            out_send.at[c, s],
            out_recv.at[c, s],
            peer,
        )

    def own_out_copy(c):
        return pltpu.make_async_copy(
            held.at[me, :, span(c * chunk, chunk)],
            out_ref.at[:, span(me * cells + c * chunk, chunk)],
            own_out.at[c],
        )

    for which in range(2):
        own_data_copy(which).start()
        each_peer(lambda s, peer: data_copy(which, s, peer).start())

    def send_members(c, carry):
        own_member_copy(c).start()
        each_peer(lambda s, peer: member_copy(c, s, peer).start())
        return carry

    own_data_copy(0).wait()
    each_peer(lambda s, peer: data_copy(0, s, peer).wait())
    piece = min(data, 256)

    def whiten(p, carry):
        here = span(p * piece, piece)
        values = response[:, :, here].astype(jnp.float32).reshape(ne, piece)
        mean = jnp.sum(values, axis=0, keepdims=True) * (1.0 / ne)
        both[:ne, here] = ((values - mean) * (scale / spread_ref[:, here])).astype(jnp.bfloat16)
        return carry

    lax.fori_loop(0, data // piece, whiten, 0)
    rows = 256

    def multiply(b, carry):
        here = span(b * rows, rows)
        sums[here, :] = lax.dot_general(
            both[here, :data], both[:ne, :data], (((1,), (1,)), ((), ())), preferred_element_type=jnp.float32
        )
        return carry

    lax.fori_loop(0, ne // rows, multiply, 0)
    own_data_copy(1).wait()
    each_peer(lambda s, peer: data_copy(1, s, peer).wait())
    lax.fori_loop(0, early, send_members, 0)

    def residual(p, carry):
        here = span(p * piece, piece)
        values = response[:, :, here].astype(jnp.float32).reshape(ne, piece)
        noise = jitter[:, :, here].astype(jnp.float32).reshape(ne, piece)
        both[ne:, here] = ((observed_ref[:, here] - values) / spread_ref[:, here] + noise).astype(
            jnp.bfloat16
        )
        return carry

    lax.fori_loop(0, data // piece, residual, 0)
    lax.fori_loop(ne // rows, 2 * ne // rows, multiply, 0)

    orders = [list(range(levels)), [0] + list(range(2, levels)) + [1]][: 2 if levels > 1 else 1]
    width = ne // len(orders)
    plans = []
    for order in orders:
        start, plan = 0, []
        for level, b in enumerate(order):
            half = ne >> level
            bit = lax.rem(me // (1 << b), 2)
            plan.append((half, start + bit * half, start + (1 - bit) * half, me + (1 - 2 * bit) * (1 << b)))
            start = start + bit * half
        plans.append(plan)

    def scatter(level, h):
        half, mine, other, partner = plans[h][level]
        columns = pl.ds(h * width, width)
        return remote(
            sums.at[span(other, half), columns],
            arrived.at[pl.ds(2 * ne - 2 * half, half), columns],
            tree_send.at[0, level, h],
            tree_recv.at[0, level, h],
            partner,
        )

    def gather(level, h):
        half, mine, other, partner = plans[h][level]
        columns = pl.ds(h * width, width)
        here = full.at[span(mine, half), columns]
        return remote(here, here, tree_send.at[1, level, h], tree_recv.at[1, level, h], partner)

    halves = range(len(orders))
    for h in halves:
        scatter(0, h).start()
    for level in range(levels):
        for h in halves:
            half, mine, other, partner = plans[h][level]
            columns = pl.ds(h * width, width)
            scatter(level, h).wait()
            total = sums[span(mine, half), columns] + arrived[pl.ds(2 * ne - 2 * half, half), columns]
            if level < levels - 1:
                sums[span(mine, half), columns] = total
                scatter(level + 1, h).start()
            else:
                full[span(mine, half), columns] = total
                gather(level, h).start()
    for level in reversed(range(levels)):
        for h in halves:
            gather(level, h).wait()
            if level:
                gather(level - 1, h).start()
    lax.fori_loop(early, count, send_members, 0)

    eye = lax.broadcasted_iota(jnp.int32, (ne, ne), 0) == lax.broadcasted_iota(
        jnp.int32, (ne, ne), 1
    )
    inverse[...] = full[:ne, :] + jnp.where(eye, damping, 0.0)

    def exact(a, b):
        return jnp.dot(a, b, precision=HIGHEST, preferred_element_type=jnp.float32)

    def step(block, carry):
        here = span(block * BLOCK, BLOCK)
        negative = sweep_block(inverse[here, here])
        column = inverse[:, here]
        scaled = -exact(negative, inverse[here, :])
        scaled_column = -exact(column, negative)
        inverse[...] = inverse[...] - exact(column, scaled)
        inverse[here, :] = scaled
        inverse[:, here] = scaled_column
        inverse[here, here] = negative
        return carry

    lax.fori_loop(0, ne // BLOCK, step, 0)
    both[:ne, :ne] = (-exact(full[ne:, :], inverse[...])).astype(jnp.bfloat16)

    def update(c, carry):
        own_member_copy(c).wait()
        each_peer(lambda s, peer: member_copy(c, s, peer).wait())
        here = span(c * chunk, chunk)
        params = params_ref[:, :, here].astype(jnp.float32).reshape(ne, chunk)
        mean = jnp.sum(params, axis=0, keepdims=True) * (1.0 / ne)
        anomaly = ((params - mean) * scale).astype(jnp.bfloat16)
        change = jnp.dot(both[:ne, :ne], anomaly, preferred_element_type=jnp.float32)
        held[:, :, here] = (params + change).reshape(n, local, chunk).astype(jnp.bfloat16)
        each_peer(lambda s, peer: out_copy(c, s, peer).start())
        own_out_copy(c).start()
        return carry

    lax.fori_loop(0, count, update, 0)

    def finish(c, carry):
        each_peer(lambda s, peer: out_copy(c, s, peer).wait())
        own_out_copy(c).wait()
        return carry

    lax.fori_loop(0, count, finish, 0)


def on_device(members, predicted, noise, observed, observation_spread):
    n = lax.axis_size("rows")
    local = members.shape[0]
    ne = local * n
    cells = members.shape[1] // n
    data = predicted.shape[1] // n
    levels = n.bit_length() - 1
    count = 4
    chunk = cells // count
    hbm = pl.BlockSpec(memory_space=pl.ANY)
    vmem = pl.BlockSpec(memory_space=pltpu.VMEM)
    dma = pltpu.SemaphoreType.DMA
    return pl.pallas_call(
        functools.partial(smoother_kernel, n, chunk, 1),
        out_shape=jax.ShapeDtypeStruct((local, n * cells), jnp.bfloat16),
        in_specs=[hbm, hbm, hbm, vmem, vmem],
        out_specs=hbm,
        scratch_shapes=[
            pltpu.VMEM((n, local, data), jnp.bfloat16),
            pltpu.VMEM((n, local, data), jnp.bfloat16),
            pltpu.VMEM((2 * ne, max(data, ne)), jnp.bfloat16),
            pltpu.VMEM((2 * ne, ne), jnp.float32),
            pltpu.VMEM((2 * ne, ne), jnp.float32),
            pltpu.VMEM((2 * ne, ne), jnp.float32),
            pltpu.VMEM((ne, ne), jnp.float32),
            pltpu.VMEM((n, local, cells), jnp.bfloat16),
            pltpu.VMEM((n, local, cells), jnp.bfloat16),
            dma((2, n)),
            dma((2, n)),
            dma((2,)),
            dma((2, levels, 2)),
            dma((2, levels, 2)),
            dma((count, n)),
            dma((count, n)),
            dma((count,)),
            dma((count, n)),
            dma((count, n)),
            dma((count,)),
        ],
        compiler_params=pltpu.CompilerParams(
            collective_id=0, has_side_effects=True, vmem_limit_bytes=50 * 2**20
        ),
        name="smoother",
    )(members, predicted, noise, observed[None], observation_spread[None])


def solution(mesh):
    in_specs = (
        P("rows", "fields"),
        P("rows", "fields"),
        P("rows", "fields"),
        P(("fields", "rows")),
        P(("fields", "rows")),
    )
    return jax.shard_map(
        on_device, mesh=mesh, in_specs=in_specs, out_specs=P("rows", "fields"), check_vma=False
    )
```

```python
import functools
import math

import jax
import jax.numpy as jnp
from jax import lax
from jax.experimental import pallas as pl
from jax.experimental.pallas import tpu as pltpu
from jax.sharding import PartitionSpec as P

damping = 21.0
BLOCK = 128
HIGHEST = lax.Precision.HIGHEST


def sweep_block(m):
    size = m.shape[0]
    rows = lax.broadcasted_iota(jnp.int32, m.shape, 0)
    columns = lax.broadcasted_iota(jnp.int32, m.shape, 1)
    lane = columns[:1]
    for k in range(0, size, 2):
        row0, row1 = m[k : k + 1, :], m[k + 1 : k + 2, :]
        column0, column1 = m[:, k : k + 1], m[:, k + 1 : k + 2]
        a, b, c = m[k : k + 1, k : k + 1], m[k : k + 1, k + 1 : k + 2], m[k + 1 : k + 2, k + 1 : k + 2]
        reciprocal = 1.0 / (a * c - b * b)
        i00, i01, i11 = c * reciprocal, -b * reciprocal, a * reciprocal
        scaled0 = jnp.where(lane == k, -i00, jnp.where(lane == k + 1, -i01, i00 * row0 + i01 * row1))
        scaled1 = jnp.where(lane == k, -i01, jnp.where(lane == k + 1, -i11, i01 * row0 + i11 * row1))
        kept = jnp.where((columns == k) | (columns == k + 1), 0.0, m)
        swept = kept - column0 * scaled0 - column1 * scaled1
        m = jnp.where(rows == k, scaled0, jnp.where(rows == k + 1, scaled1, swept))
    return m


MESH = pl.DeviceIdType.MESH


def smoother_kernel(
    n,
    chunk,
    early,
    members_ref,
    predicted_ref,
    noise_ref,
    observed_ref,
    spread_ref,
    out_ref,
    response,
    jitter,
    both,
    sums,
    arrived,
    full,
    inverse,
    params_ref,
    held,
    data_send,
    data_recv,
    own_data,
    tree_send,
    tree_recv,
    member_send,
    member_recv,
    own_member,
    out_send,
    out_recv,
    own_out,
):
    me = lax.axis_index("rows")
    local = members_ref.shape[0]
    ne = n * local
    cells = members_ref.shape[1] // n
    data = predicted_ref.shape[1] // n
    count = cells // chunk
    levels = n.bit_length() - 1
    scale = 1.0 / math.sqrt(ne - 1)
    barrier = pltpu.get_barrier_semaphore()

    def each_peer(do):
        def one(s, carry):
            do(s, lax.rem(me + s, n))
            return carry

        lax.fori_loop(1, n, one, 0)

    def span(start, size):
        return pl.ds(pl.multiple_of(start, size), size)

    each_peer(
        lambda s, peer: pl.semaphore_signal(
            barrier, inc=1, device_id={"rows": peer}, device_id_type=MESH
        )
    )
    pl.semaphore_wait(barrier, n - 1)

    def remote(source, target, send, recv, peer):
        return pltpu.make_async_remote_copy(
            src_ref=source,
            dst_ref=target,
            send_sem=send,
            recv_sem=recv,
            device_id={"rows": peer},
            device_id_type=MESH,
        )

    fields = ((predicted_ref, response), (noise_ref, jitter))

    def data_copy(which, s, peer):
        source, target = fields[which]
        return remote(
            source.at[:, span(peer * data, data)],
            target.at[me],
            data_send.at[which, s],
            data_recv.at[which, s],
            peer,
        )

    def own_data_copy(which):
        source, target = fields[which]
        return pltpu.make_async_copy(
            source.at[:, span(me * data, data)], target.at[me], own_data.at[which]
        )

    def member_copy(c, s, peer):
        return remote(
            members_ref.at[:, span(peer * cells + c * chunk, chunk)],
            params_ref.at[me, :, span(c * chunk, chunk)],
            member_send.at[c, s],
            member_recv.at[c, s],
            peer,
        )

    def own_member_copy(c):
        return pltpu.make_async_copy(
            members_ref.at[:, span(me * cells + c * chunk, chunk)],
            params_ref.at[me, :, span(c * chunk, chunk)],
            own_member.at[c],
        )

    def out_copy(c, s, peer):
        return remote(
            held.at[peer, :, span(c * chunk, chunk)],
            out_ref.at[:, span(me * cells + c * chunk, chunk)],
            out_send.at[c, s],
            out_recv.at[c, s],
            peer,
        )

    def own_out_copy(c):
        return pltpu.make_async_copy(
            held.at[me, :, span(c * chunk, chunk)],
            out_ref.at[:, span(me * cells + c * chunk, chunk)],
            own_out.at[c],
        )

    for c in range(count):
        own_member_copy(c).start()
    for which in range(2):
        own_data_copy(which).start()
        each_peer(lambda s, peer: data_copy(which, s, peer).start())

    slugs = 4 * count
    part = chunk // 4

    def send_members(slug, carry):
        c = slug // 4
        offset = c * chunk + lax.rem(slug, 4) * part

        def one(s, peer):
            remote(
                members_ref.at[:, span(peer * cells + offset, part)],
                params_ref.at[me, :, span(offset, part)],
                member_send.at[c, s],
                member_recv.at[c, s],
                peer,
            ).start()

        each_peer(one)
        return carry

    sent = 0

    def slip_members(more):
        nonlocal sent
        more = min(more, slugs - sent)
        if more:
            lax.fori_loop(sent, sent + more, send_members, 0)
        sent += more

    own_data_copy(0).wait()
    each_peer(lambda s, peer: data_copy(0, s, peer).wait())
    piece = min(data, 256)

    def whiten(p, carry):
        here = span(p * piece, piece)
        values = response[:, :, here].astype(jnp.float32).reshape(ne, piece)
        mean = jnp.sum(values, axis=0, keepdims=True) * (1.0 / ne)
        both[:ne, here] = ((values - mean) * (scale / spread_ref[:, here])).astype(jnp.bfloat16)
        return carry

    lax.fori_loop(0, data // piece, whiten, 0)
    rows = 256

    def multiply(b, carry):
        here = span(b * rows, rows)
        sums[here, :] = lax.dot_general(
            both[here, :data], both[:ne, :data], (((1,), (1,)), ((), ())), preferred_element_type=jnp.float32
        )
        return carry

    lax.fori_loop(0, ne // rows, multiply, 0)
    own_data_copy(1).wait()
    each_peer(lambda s, peer: data_copy(1, s, peer).wait())
    slip_members(early)

    def residual(p, carry):
        here = span(p * piece, piece)
        values = response[:, :, here].astype(jnp.float32).reshape(ne, piece)
        noise = jitter[:, :, here].astype(jnp.float32).reshape(ne, piece)
        both[ne:, here] = ((observed_ref[:, here] - values) / spread_ref[:, here] + noise).astype(
            jnp.bfloat16
        )
        return carry

    lax.fori_loop(0, data // piece, residual, 0)
    lax.fori_loop(ne // rows, 2 * ne // rows, multiply, 0)

    orders = [list(range(levels)), [0] + list(range(2, levels)) + [1]][: 2 if levels > 1 else 1]
    width = ne // len(orders)
    plans = []
    for order in orders:
        start, plan = 0, []
        for level, b in enumerate(order):
            half = ne >> level
            bit = lax.rem(me // (1 << b), 2)
            plan.append((half, start + bit * half, start + (1 - bit) * half, me + (1 - 2 * bit) * (1 << b)))
            start = start + bit * half
        plans.append(plan)

    def scatter(level, h):
        half, mine, other, partner = plans[h][level]
        columns = pl.ds(h * width, width)
        return remote(
            sums.at[span(other, half), columns],
            arrived.at[pl.ds(2 * ne - 2 * half, half), columns],
            tree_send.at[0, level, h],
            tree_recv.at[0, level, h],
            partner,
        )

    def gather(level, h):
        half, mine, other, partner = plans[h][level]
        columns = pl.ds(h * width, width)
        here = full.at[span(mine, half), columns]
        return remote(here, here, tree_send.at[1, level, h], tree_recv.at[1, level, h], partner)

    halves = range(len(orders))
    for h in halves:
        scatter(0, h).start()
    for level in range(levels):
        for h in halves:
            half, mine, other, partner = plans[h][level]
            columns = pl.ds(h * width, width)
            scatter(level, h).wait()
            total = sums[span(mine, half), columns] + arrived[pl.ds(2 * ne - 2 * half, half), columns]
            if level < levels - 1:
                sums[span(mine, half), columns] = total
                scatter(level + 1, h).start()
            else:
                full[span(mine, half), columns] = total
                gather(level, h).start()
        slip_members(1)
    for level in reversed(range(levels)):
        for h in halves:
            gather(level, h).wait()
            if level:
                gather(level - 1, h).start()
        if level:
            slip_members(1)
    slip_members(slugs)

    eye = lax.broadcasted_iota(jnp.int32, (ne, ne), 0) == lax.broadcasted_iota(
        jnp.int32, (ne, ne), 1
    )
    inverse[...] = full[:ne, :] + jnp.where(eye, damping, 0.0)

    def exact(a, b):
        return jnp.dot(a, b, precision=HIGHEST, preferred_element_type=jnp.float32)

    def step(block, carry):
        here = span(block * BLOCK, BLOCK)
        negative = sweep_block(inverse[here, here])
        column = inverse[:, here]
        scaled = -exact(negative, inverse[here, :])
        scaled_column = -exact(column, negative)
        inverse[...] = inverse[...] - exact(column, scaled)
        inverse[here, :] = scaled
        inverse[:, here] = scaled_column
        inverse[here, here] = negative
        return carry

    lax.fori_loop(0, ne // BLOCK, step, 0)
    both[:ne, :ne] = (-exact(full[ne:, :], inverse[...])).astype(jnp.bfloat16)

    def update(c, carry):
        own_member_copy(c).wait()
        each_peer(lambda s, peer: member_copy(c, s, peer).wait())
        here = span(c * chunk, chunk)
        params = params_ref[:, :, here].astype(jnp.float32).reshape(ne, chunk)
        mean = jnp.sum(params, axis=0, keepdims=True) * (1.0 / ne)
        anomaly = ((params - mean) * scale).astype(jnp.bfloat16)
        change = jnp.dot(both[:ne, :ne], anomaly, preferred_element_type=jnp.float32)
        held[:, :, here] = (params + change).reshape(n, local, chunk).astype(jnp.bfloat16)
        each_peer(lambda s, peer: out_copy(c, s, peer).start())
        own_out_copy(c).start()
        return carry

    lax.fori_loop(0, count, update, 0)

    def finish(c, carry):
        each_peer(lambda s, peer: out_copy(c, s, peer).wait())
        own_out_copy(c).wait()
        return carry

    lax.fori_loop(0, count, finish, 0)


def on_device(members, predicted, noise, observed, observation_spread):
    n = lax.axis_size("rows")
    local = members.shape[0]
    ne = local * n
    cells = members.shape[1] // n
    data = predicted.shape[1] // n
    levels = n.bit_length() - 1
    count = 4
    chunk = cells // count
    hbm = pl.BlockSpec(memory_space=pl.ANY)
    vmem = pl.BlockSpec(memory_space=pltpu.VMEM)
    dma = pltpu.SemaphoreType.DMA
    return pl.pallas_call(
        functools.partial(smoother_kernel, n, chunk, 1),
        out_shape=jax.ShapeDtypeStruct((local, n * cells), jnp.bfloat16),
        in_specs=[hbm, hbm, hbm, vmem, vmem],
        out_specs=hbm,
        scratch_shapes=[
            pltpu.VMEM((n, local, data), jnp.bfloat16),
            pltpu.VMEM((n, local, data), jnp.bfloat16),
            pltpu.VMEM((2 * ne, max(data, ne)), jnp.bfloat16),
            pltpu.VMEM((2 * ne, ne), jnp.float32),
            pltpu.VMEM((2 * ne, ne), jnp.float32),
            pltpu.VMEM((2 * ne, ne), jnp.float32),
            pltpu.VMEM((ne, ne), jnp.float32),
            pltpu.VMEM((n, local, cells), jnp.bfloat16),
            pltpu.VMEM((n, local, cells), jnp.bfloat16),
            dma((2, n)),
            dma((2, n)),
            dma((2,)),
            dma((2, levels, 2)),
            dma((2, levels, 2)),
            dma((count, n)),
            dma((count, n)),
            dma((count,)),
            dma((count, n)),
            dma((count, n)),
            dma((count,)),
        ],
        compiler_params=pltpu.CompilerParams(
            collective_id=0, has_side_effects=True, vmem_limit_bytes=50 * 2**20
        ),
        name="smoother",
    )(members, predicted, noise, observed[None], observation_spread[None])


def solution(mesh):
    in_specs = (
        P("rows", "fields"),
        P("rows", "fields"),
        P("rows", "fields"),
        P(("fields", "rows")),
        P(("fields", "rows")),
    )
    return jax.shard_map(
        on_device, mesh=mesh, in_specs=in_specs, out_specs=P("rows", "fields"), check_vma=False
    )
```
